768 devices in a mesh: rep: 8 (over y_lo, core), shard: 96 (over y_hi, x, z).
Axes of the slice: x: 4, y: 8 (y_hi: 2, y_lo: 4; y = y_hi * 4 + y_lo), z: 12, core: 2. Of those that a mesh axis runs over, the one named last changes fastest.
Arguments:
- delta: bfloat16 [8, 6144, 6144], P('rep', 'shard'), may hold values from -11 to 11
- counts: int32 [8], replicated, may hold values from 1000 to 7999
- params: bfloat16 [6144, 6144], P('shard'), may hold values from -0.078125 to 0.078125
- momentum: float32 [6144, 6144], P('shard', 'rep'), may hold values from -4 to 4
Outputs:
- new_params: bfloat16 [6144, 6144], P('shard')
- new_momentum: float32 [6144, 6144], P('shard', 'rep')
- update_rms: float32 [], replicated
- mean_variance: float32 [], replicated
The draws below stay inside these ranges and needn't reach their ends.
All inputs are finite; a program needn't handle non-finite values.
Results may differ from the reference program's by a relative error of at most 0.0004.
Values may be sent and summed in bfloat16 or wider, within the bound.
No kernel may reach another device: no remote copies, remote signals or barrier semaphores. Data moves between devices by JAX's collectives and lax.ppermute only.
A program may use at most 32 MiB of HBM per device.

```python
import jax
import jax.numpy as jnp

D = 6144
ROWS_DEV = 64
ROWS = 6144
N_REP = 8


def draw_delta(key, part):
    first_key = jax.random.fold_in(key, 0)
    row_key = jax.random.fold_in(key, 3)
    block_key = jax.random.fold_in(key, 4)
    row_scale = jnp.exp(jax.random.uniform(row_key, (ROWS,), jnp.float32, -1.0, 1.0))
    block_count = ROWS // ROWS_DEV
    column_width = D // N_REP
    block_factor = jnp.exp(jax.random.uniform(block_key, (N_REP, block_count, N_REP), jnp.float32, -0.7, 0.7))
    values = jax.random.truncated_normal(first_key, -6.0, 6.0, (N_REP, ROWS, D), jnp.float32)
    values = values * row_scale[None, :, None]
    shaped = values.reshape(N_REP, block_count, ROWS_DEV, N_REP, column_width)
    shaped = shaped * block_factor[:, :, None, :, None]
    values = jnp.clip(shaped.reshape(N_REP, ROWS, D), -11.0, 11.0)
    return values.astype(jnp.bfloat16)


def touch_ends(array, rng, low, top_value):
    index_at = [jax.random.randint(jax.random.fold_in(rng, axis), (), 0, length) for axis, length in enumerate(array.shape)]
    widest = array.shape.index(max(array.shape))
    next_to = index_at[:widest] + [(index_at[widest] + 1) % array.shape[widest]] + index_at[widest + 1:]
    return array.at[tuple(index_at)].set(low).at[tuple(next_to)].set(top_value)


def steps_of(own_key, dims, pieces, least, largest):
    def one(dim, blocks):
        heights = jax.random.uniform(jax.random.fold_in(jax.random.fold_in(own_key, 6), dim), (blocks,), jnp.float32, least / len(pieces), largest / len(pieces))
        return jnp.repeat(jnp.exp(heights), dims[dim] // blocks).reshape((-1,) + (1,) * (len(dims) - dim - 1))

    level = one(*pieces[0])
    for cut in pieces[1:]:
        level = level * one(*cut)
    return level


def normal_values(stream_key, dims, width, most, shards=(), held_as=jnp.bfloat16):
    drawn = jax.random.normal(stream_key, dims, jnp.float32) * width
    if len(shards) > 0:
        drawn = steps_of(stream_key, dims, shards, -0.22, 0.18) * drawn
    return jnp.clip(drawn, min=-most, max=most).astype(held_as)


def setup_inputs(seed: int = 0) -> dict:
    key_list = jax.random.split(jax.random.key(seed), 5)
    delta = draw_delta(jax.random.fold_in(key_list[4], 71), 0)
    counts = touch_ends(jax.random.randint(key_list[1], (N_REP,), 1000, 8000), jax.random.fold_in(key_list[1], 1), 1000, 7999).astype(jnp.int32)
    params = normal_values(key_list[2], (ROWS, D), D ** -0.5, 0.078125, ((0, 96),))
    momentum = normal_values(key_list[3], (ROWS, D), 0.3, 4.0, ((0, 96), (1, 8)), jnp.float32)
    return dict(delta=delta, counts=counts, params=params, momentum=momentum)


clip_rms = 0.2
beta_outer = 0.9
outer_rate = 0.7
epsilon = 1e-06

def reference(delta, counts, params, momentum):
    tokens = counts.astype(jnp.float32)
    weights = tokens / jnp.sum(tokens)
    mean_delta = jnp.zeros((ROWS, D), jnp.float32)
    for replica in range(N_REP):
        mean_delta = mean_delta + weights[replica] * delta[replica].astype(jnp.float32)
    variance = jnp.zeros((ROWS, D), jnp.float32)
    for replica in range(N_REP):
        centered = delta[replica].astype(jnp.float32) - mean_delta
        variance = variance + weights[replica] * centered * centered
    element_count = ROWS * D
    update_rms = jnp.sqrt(jnp.sum(mean_delta * mean_delta) / element_count)
    mean_variance = jnp.sum(variance) / element_count
    clip_factor = clip_rms / jnp.maximum(update_rms, clip_rms)
    damped = clip_factor * mean_delta / (1.0 + variance / (mean_variance + epsilon))
    new_momentum = beta_outer * momentum + damped
    outer_update = outer_rate * (damped + beta_outer * new_momentum)
    new_params = (params.astype(jnp.float32) - outer_update).astype(jnp.bfloat16)
    return (new_params, new_momentum, update_rms, mean_variance)
```

```python
import jax
import jax.numpy as jnp
from jax import lax
from jax.sharding import Mesh
from jax.sharding import PartitionSpec as P

REP = ("rep_0", "rep_1")
SHARD = ("shard_0", "shard_1", "shard_2")
SUM_STAGES = (("shard_2", "rep_1"), ("shard_1", "shard_0", "rep_0"))

clip_rms = 0.2
beta_outer = 0.9
outer_rate = 0.7
epsilon = 1e-06


def in_column_blocks(shard, length):
    rows, columns = shard.shape
    return jnp.moveaxis(shard.reshape(rows, length, columns // length), 1, 0)


def summed_over(values, axes):
    copies = jnp.broadcast_to(values[None], (lax.axis_size(axes), *values.shape))
    return jnp.sum(lax.all_to_all(copies, axes, 0, 0, tiled=True), axis=0)


def shards(delta, counts, params, momentum):
    replica_index = lax.axis_index(REP)
    tokens = counts.astype(jnp.float32)
    weights = (tokens / jnp.sum(tokens))[:, None, None]
    block_width = momentum.shape[1]
    blocks = in_column_blocks(delta[0], lax.axis_size(REP))
    blocks = lax.all_to_all(blocks, REP, 0, 0, tiled=True)
    own_params = lax.dynamic_slice_in_dim(params, replica_index * block_width, block_width, 1)
    blocks, own_params = lax.optimization_barrier((blocks, own_params.astype(jnp.float32)))
    wide_blocks = blocks.astype(jnp.float32)
    mean_block = jnp.sum(weights * wide_blocks, axis=0)
    deviation = wide_blocks - mean_block[None]
    variance = jnp.sum(weights * (deviation * deviation), axis=0)
    totals = jnp.stack([jnp.sum(mean_block * mean_block), jnp.sum(variance)])
    for axes in SUM_STAGES:
        totals = summed_over(totals, axes)
    element_count = mean_block.size * lax.axis_size(REP) * lax.axis_size(SHARD)
    update_rms = jnp.sqrt(totals[0] / element_count)
    mean_variance = totals[1] / element_count
    clip_factor = clip_rms / jnp.maximum(update_rms, clip_rms)
    damped = clip_factor * mean_block / (1.0 + variance / (mean_variance + epsilon))
    new_momentum = beta_outer * momentum + damped
    outer_update = outer_rate * (damped + beta_outer * new_momentum)
    new_block = (own_params - outer_update).astype(jnp.bfloat16)
    new_params = lax.all_gather(new_block, REP, axis=1, tiled=True)
    return (new_params, new_momentum, update_rms, mean_variance)


def solution(mesh):
    finer = Mesh(
        mesh.devices.reshape(4, 2, 2, 4, 12), ("rep_0", "rep_1", "shard_0", "shard_1", "shard_2")
    )
    in_specs = (P(REP, SHARD, None), P(), P(SHARD, None), P(SHARD, REP))
    out_specs = (P(SHARD, None), P(SHARD, REP), P(), P())
    return jax.shard_map(
        shards, mesh=finer, in_specs=in_specs, out_specs=out_specs, check_vma=False
    )
```

```python
import functools

import jax
import jax.numpy as jnp
from jax import lax
from jax.experimental import pallas as pl
from jax.experimental.pallas import tpu as pltpu
from jax.sharding import Mesh
from jax.sharding import PartitionSpec as P

REP = ("rep_0", "rep_1")
SHARD = ("shard_0", "shard_1", "shard_2")
SUM_STAGES = (("shard_2", "rep_1"), ("shard_1", "shard_0", "rep_0"))
LANES = 128
CHUNK_ROWS = 32

clip_rms = 0.2
beta_outer = 0.9
outer_rate = 0.7
epsilon = 1e-06

VMEM = pl.BlockSpec(memory_space=pltpu.VMEM)
SMEM = pl.BlockSpec(memory_space=pltpu.SMEM)
HBM = pl.BlockSpec(memory_space=pltpu.MemorySpace.HBM)
SMALL = pltpu.CompilerParams(vmem_limit_bytes=8 * 1024 * 1024)


def chunks(rows, columns):
    for column in range(0, columns, LANES):
        for row in range(0, rows, CHUNK_ROWS):
            yield pl.ds(row, CHUNK_ROWS), pl.ds(column, LANES)


def total(values):
    values = list(values)
    while len(values) > 1:
        values = [sum(values[i : i + 2]) for i in range(0, len(values), 2)]
    return values[0]


def to_sublanes(values):
    return total(values[i : i + 8] for i in range(0, values.shape[0], 8))


def split_kernel(
    counts_hbm, delta_ref, params_ref, blocks_ref, own_ref, weights_ref, counts_ref, sems
):
    length, _, width = blocks_ref.shape
    mine = lax.axis_index(REP)
    copies = [
        pltpu.make_async_copy(
            delta_ref.at[0, :, pl.ds(r * width, width)], blocks_ref.at[r], sems.at[r]
        )
        for r in range(length)
    ]
    own_columns = pl.ds(pl.multiple_of(mine * width, LANES), width)
    copies.append(pltpu.make_async_copy(params_ref.at[:, own_columns], own_ref, sems.at[length]))
    counts_copy = pltpu.make_async_copy(counts_hbm, counts_ref, sems.at[length + 1])
    counts_copy.start()
    for copy in copies:
        copy.start()
    counts_copy.wait()
    row = lax.broadcasted_iota(jnp.int32, weights_ref.shape, 0)
    tokens = jnp.zeros(weights_ref.shape, jnp.float32)
    for r in range(length):
        tokens = jnp.where(row == r, counts_ref[r].astype(jnp.float32), tokens)
    all_tokens = total(counts_ref[r] for r in range(length)).astype(jnp.float32)
    weights_ref[...] = tokens / all_tokens
    for copy in copies:
        copy.wait()


def moments_kernel(blocks_ref, weights_ref, mean_ref, variance_ref, totals_ref):
    length, rows, columns = blocks_ref.shape
    weights = [
        jnp.broadcast_to(weights_ref[pl.ds(r, 1), :], (CHUNK_ROWS, LANES)) for r in range(length)
    ]
    squares, variances = [], []
    for where in chunks(rows, columns):
        values = [blocks_ref[(r, *where)].astype(jnp.float32) for r in range(length)]
        mean = total(w * v for w, v in zip(weights, values))
        deviations = [v - mean for v in values]
        variance = total(w * (d * d) for w, d in zip(weights, deviations))
        mean_ref[where] = mean
        variance_ref[where] = variance
        squares.append(to_sublanes(mean * mean))
        variances.append(to_sublanes(variance))
    square_row = jnp.sum(total(squares), axis=0, keepdims=True)
    variance_row = jnp.sum(total(variances), axis=0, keepdims=True)
    which = lax.broadcasted_iota(jnp.int32, (2, LANES), 0)
    both = jnp.where(which == 0, square_row, variance_row)
    totals_ref[...] = jnp.broadcast_to(both[None], totals_ref.shape)


def update_kernel(
    element_count,
    totals_ref,
    mean_ref,
    variance_ref,
    own_ref,
    momentum_ref,
    block_ref,
    new_momentum_ref,
    update_rms_ref,
    mean_variance_ref,
):
    totals = jnp.sum(jnp.sum(totals_ref[...], axis=0), axis=1, keepdims=True)
    update_rms = jnp.sqrt(totals[0:1] / element_count)
    mean_variance = totals[1:2] / element_count
    update_rms_ref[0] = update_rms[0, 0]
    mean_variance_ref[0] = mean_variance[0, 0]
    clip_factor = clip_rms / jnp.maximum(update_rms, clip_rms)
    scale = mean_variance + epsilon
    for where in chunks(*mean_ref.shape):
        damped = clip_factor * mean_ref[where] / (1.0 + variance_ref[where] / scale)
        new_momentum = beta_outer * momentum_ref[where] + damped
        new_momentum_ref[where] = new_momentum
        outer_update = outer_rate * (damped + beta_outer * new_momentum)
        block_ref[where] = (own_ref[where].astype(jnp.float32) - outer_update).astype(jnp.bfloat16)


def copies_for(values, axes):
    return jnp.broadcast_to(values[None], (lax.axis_size(axes), *values.shape))


def shards(delta, counts, params, momentum):
    length = lax.axis_size(REP)
    rows, width = momentum.shape
    shape = functools.partial(jax.ShapeDtypeStruct, (rows, width))
    blocks, own_params, weights = pl.pallas_call(
        split_kernel,
        in_specs=[HBM] * 3,
        out_specs=[VMEM] * 3,
        out_shape=[
            jax.ShapeDtypeStruct((length, rows, width), delta.dtype),
            shape(params.dtype),
            jax.ShapeDtypeStruct((length, LANES), jnp.float32),
        ],
        scratch_shapes=[pltpu.SMEM(counts.shape, counts.dtype), pltpu.SemaphoreType.DMA((length + 2,))],
        compiler_params=SMALL,
    )(counts, delta, params)
    blocks = lax.all_to_all(blocks, REP, 0, 0, tiled=True)
    first, second = SUM_STAGES
    mean, variance, totals = pl.pallas_call(
        moments_kernel,
        in_specs=[VMEM] * 2,
        out_specs=[VMEM] * 3,
        out_shape=[
            shape(jnp.float32),
            shape(jnp.float32),
            jax.ShapeDtypeStruct((lax.axis_size(first), 2, LANES), jnp.float32),
        ],
        compiler_params=SMALL,
    )(blocks, weights)
    totals = lax.all_to_all(totals, first, 0, 0, tiled=True)
    totals = copies_for(jnp.sum(totals, axis=0), second)
    totals = lax.all_to_all(totals, second, 0, 0, tiled=True)
    element_count = rows * width * length * lax.axis_size(SHARD)
    new_block, new_momentum, update_rms, mean_variance = pl.pallas_call(
        functools.partial(update_kernel, element_count),
        in_specs=[VMEM] * 5,
        out_specs=[VMEM, VMEM, SMEM, SMEM],
        out_shape=[
            shape(params.dtype),
            shape(jnp.float32),
            jax.ShapeDtypeStruct((1,), jnp.float32),
            jax.ShapeDtypeStruct((1,), jnp.float32),
        ],
        compiler_params=SMALL,
    )(totals, mean, variance, own_params, momentum)
    new_params = lax.all_gather(new_block, REP, axis=1, tiled=True)
    return (new_params, new_momentum, update_rms[0], mean_variance[0])


def solution(mesh):
    finer = Mesh(
        mesh.devices.reshape(4, 2, 2, 4, 12), ("rep_0", "rep_1", "shard_0", "shard_1", "shard_2")
    )
    in_specs = (P(REP, SHARD, None), P(), P(SHARD, None), P(SHARD, REP))
    out_specs = (P(SHARD, None), P(SHARD, REP), P(), P())
    return jax.shard_map(
        shards, mesh=finer, in_specs=in_specs, out_specs=out_specs, check_vma=False
    )
```

```python
import functools

import jax
import jax.numpy as jnp
from jax import lax
from jax.experimental import pallas as pl
from jax.experimental.pallas import tpu as pltpu
from jax.sharding import Mesh
from jax.sharding import PartitionSpec as P

REP = ("rep_0", "rep_1")
SHARD = ("shard_0", "shard_1", "shard_2")
SUM_STAGES = (("shard_2", "rep_1"), ("shard_1", "shard_0", "rep_0"))
LANES = 128
CHUNK_ROWS = 32

clip_rms = 0.2
beta_outer = 0.9
outer_rate = 0.7
epsilon = 1e-06

VMEM = pl.BlockSpec(memory_space=pltpu.VMEM)
SMEM = pl.BlockSpec(memory_space=pltpu.SMEM)
HBM = pl.BlockSpec(memory_space=pltpu.MemorySpace.HBM)
SMALL = pltpu.CompilerParams(vmem_limit_bytes=8 * 1024 * 1024)


def chunks(rows, columns):
    for column in range(0, columns, LANES):
        for row in range(0, rows, CHUNK_ROWS):
            yield pl.ds(row, CHUNK_ROWS), pl.ds(column, LANES)


def total(values):
    values = list(values)
    while len(values) > 1:
        values = [sum(values[i : i + 2]) for i in range(0, len(values), 2)]
    return values[0]


def to_sublanes(values):
    return total(values[i : i + 8] for i in range(0, values.shape[0], 8))


def split_kernel(
    counts_hbm, delta_ref, params_ref, blocks_ref, own_ref, weights_ref, counts_ref, sems
):
    length, _, width = blocks_ref.shape
    mine = lax.axis_index(REP)
    copies = [
        pltpu.make_async_copy(
            delta_ref.at[0, :, pl.ds(r * width, width)], blocks_ref.at[r], sems.at[r]
        )
        for r in range(length)
    ]
    own_columns = pl.ds(pl.multiple_of(mine * width, LANES), width)
    copies.append(pltpu.make_async_copy(params_ref.at[:, own_columns], own_ref, sems.at[length]))
    counts_copy = pltpu.make_async_copy(counts_hbm, counts_ref, sems.at[length + 1])
    counts_copy.start()
    for copy in copies:
        copy.start()
    counts_copy.wait()
    row = lax.broadcasted_iota(jnp.int32, weights_ref.shape, 0)
    tokens = jnp.zeros(weights_ref.shape, jnp.float32)
    for r in range(length):
        tokens = jnp.where(row == r, counts_ref[r].astype(jnp.float32), tokens)
    all_tokens = total(counts_ref[r] for r in range(length)).astype(jnp.float32)
    weights_ref[...] = tokens / all_tokens
    for copy in copies:
        copy.wait()


def moments_kernel(blocks_ref, weights_ref, mean_ref, variance_ref, totals_ref):
    length, rows, columns = blocks_ref.shape
    weights = [
        jnp.broadcast_to(weights_ref[pl.ds(r, 1), :], (CHUNK_ROWS, LANES)) for r in range(length)
    ]
    squares, variances = [], []
    for where in chunks(rows, columns):
        values = [blocks_ref[(r, *where)].astype(jnp.float32) for r in range(length)]
        mean = total(w * v for w, v in zip(weights, values))
        deviations = [v - mean for v in values]
        variance = total(w * (d * d) for w, d in zip(weights, deviations))
        mean_ref[where] = mean
        variance_ref[where] = variance
        squares.append(to_sublanes(mean * mean))
        variances.append(to_sublanes(variance))
    square_row = jnp.sum(total(squares), axis=0, keepdims=True)
    variance_row = jnp.sum(total(variances), axis=0, keepdims=True)
    which = lax.broadcasted_iota(jnp.int32, (2, LANES), 0)
    both = jnp.where(which == 0, square_row, variance_row)
    totals_ref[...] = jnp.broadcast_to(both[None], totals_ref.shape)


def update_kernel(
    element_count,
    totals_ref,
    mean_ref,
    variance_ref,
    own_ref,
    momentum_ref,
    block_ref,
    new_momentum_ref,
    update_rms_ref,
    mean_variance_ref,
):
    totals = jnp.sum(jnp.sum(totals_ref[...], axis=0), axis=1, keepdims=True)
    update_rms = jnp.sqrt(totals[0:1] / element_count)
    mean_variance = totals[1:2] / element_count
    update_rms_ref[0] = update_rms[0, 0]
    mean_variance_ref[0] = mean_variance[0, 0]
    clip_factor = clip_rms / jnp.maximum(update_rms, clip_rms)
    scale = mean_variance + epsilon
    for where in chunks(*mean_ref.shape):
        damped = clip_factor * mean_ref[where] / (1.0 + variance_ref[where] / scale)
        new_momentum = beta_outer * momentum_ref[where] + damped
        new_momentum_ref[where] = new_momentum
        outer_update = outer_rate * (damped + beta_outer * new_momentum)
        block_ref[where] = (own_ref[where].astype(jnp.float32) - outer_update).astype(jnp.bfloat16)


def copies_for(values, axes):
    return jnp.broadcast_to(values[None], (lax.axis_size(axes), *values.shape))


def shards(delta, counts, params, momentum):
    length = lax.axis_size(REP)
    rows, width = momentum.shape
    shape = functools.partial(jax.ShapeDtypeStruct, (rows, width))
    counts, delta, params = [
        pltpu.with_memory_space_constraint(a, pltpu.MemorySpace.HBM)
        for a in (counts, delta, params)
    ]
    blocks, own_params, weights = pl.pallas_call(
        split_kernel,
        in_specs=[HBM] * 3,
        out_specs=[VMEM] * 3,
        out_shape=[
            jax.ShapeDtypeStruct((length, rows, width), delta.dtype),
            shape(params.dtype),
            jax.ShapeDtypeStruct((length, LANES), jnp.float32),
        ],
        scratch_shapes=[pltpu.SMEM(counts.shape, counts.dtype), pltpu.SemaphoreType.DMA((length + 2,))],
        compiler_params=SMALL,
    )(counts, delta, params)
    blocks = lax.all_to_all(blocks, REP, 0, 0, tiled=True)
    first, second = SUM_STAGES
    mean, variance, totals = pl.pallas_call(
        moments_kernel,
        in_specs=[VMEM] * 2,
        out_specs=[VMEM] * 3,
        out_shape=[
            shape(jnp.float32),
            shape(jnp.float32),
            jax.ShapeDtypeStruct((lax.axis_size(first), 2, LANES), jnp.float32),
        ],
        compiler_params=SMALL,
    )(blocks, weights)
    totals = lax.all_to_all(totals, first, 0, 0, tiled=True)
    totals = copies_for(jnp.sum(totals, axis=0), second)
    totals = lax.all_to_all(totals, second, 0, 0, tiled=True)
    element_count = rows * width * length * lax.axis_size(SHARD)
    new_block, new_momentum, update_rms, mean_variance = pl.pallas_call(
        functools.partial(update_kernel, element_count),
        in_specs=[VMEM] * 5,
        out_specs=[VMEM, VMEM, SMEM, SMEM],
        out_shape=[
            shape(params.dtype),
            shape(jnp.float32),
            jax.ShapeDtypeStruct((1,), jnp.float32),
            jax.ShapeDtypeStruct((1,), jnp.float32),
        ],
        compiler_params=SMALL,
    )(totals, mean, variance, own_params, momentum)
    new_params = lax.all_gather(new_block, REP, axis=1, tiled=True)
    return (new_params, new_momentum, update_rms[0], mean_variance[0])


def solution(mesh):
    finer = Mesh(
        mesh.devices.reshape(4, 2, 2, 4, 12), ("rep_0", "rep_1", "shard_0", "shard_1", "shard_2")
    )
    in_specs = (P(REP, SHARD, None), P(), P(SHARD, None), P(SHARD, REP))
    out_specs = (P(SHARD, None), P(SHARD, REP), P(), P())
    return jax.shard_map(
        shards, mesh=finer, in_specs=in_specs, out_specs=out_specs, check_vma=False
    )
```

```python
import functools

import jax
import jax.numpy as jnp
from jax import lax
from jax.experimental import pallas as pl
from jax.experimental.pallas import tpu as pltpu
from jax.sharding import Mesh
from jax.sharding import PartitionSpec as P

REP = ("rep_0", "rep_1")
SHARD = ("shard_0", "shard_1", "shard_2")
SUM_STAGES = (("shard_2", "rep_1"), ("shard_1", "shard_0", "rep_0"))
LANES = 128
HALF = LANES // 2
STORES = 4
CHUNK_ROWS = 32

clip_rms = 0.2
beta_outer = 0.9
outer_rate = 0.7
epsilon = 1e-06

VMEM = pl.BlockSpec(memory_space=pltpu.VMEM)
HBM = pl.BlockSpec(memory_space=pltpu.MemorySpace.HBM)
SMALL = pltpu.CompilerParams(vmem_limit_bytes=8 * 1024 * 1024)


def chunks(rows, columns):
    for column in range(0, columns, LANES):
        for row in range(0, rows, CHUNK_ROWS):
            yield pl.ds(row, CHUNK_ROWS), pl.ds(column, LANES)


def total(values):
    values = list(values)
    while len(values) > 1:
        values = [sum(values[i : i + 2]) for i in range(0, len(values), 2)]
    return values[0]


def to_sublanes(values):
    return total(values[i : i + 8] for i in range(0, values.shape[0], 8))


def split_kernel(
    counts_hbm, delta_ref, params_ref, blocks_ref, own_ref, weights_ref, counts_ref, sems
):
    length, _, width = blocks_ref.shape
    mine = lax.axis_index(REP)
    copies = [
        pltpu.make_async_copy(
            delta_ref.at[0, :, pl.ds(r * width, width)], blocks_ref.at[r], sems.at[r]
        )
        for r in range(length)
    ]
    own_columns = pl.ds(pl.multiple_of(mine * width, LANES), width)
    copies.append(pltpu.make_async_copy(params_ref.at[:, own_columns], own_ref, sems.at[length]))
    counts_copy = pltpu.make_async_copy(counts_hbm, counts_ref, sems.at[length + 1])
    counts_copy.start()
    for copy in copies:
        copy.start()
    counts_copy.wait()
    row = lax.broadcasted_iota(jnp.int32, weights_ref.shape, 0)
    tokens = jnp.zeros(weights_ref.shape, jnp.float32)
    for r in range(length):
        tokens = jnp.where(row == r, counts_ref[r].astype(jnp.float32), tokens)
    all_tokens = total(counts_ref[r] for r in range(length)).astype(jnp.float32)
    weights_ref[...] = tokens / all_tokens
    for copy in copies:
        copy.wait()


def moments_kernel(blocks_ref, weights_ref, mean_ref, variance_ref, totals_ref):
    length, rows, columns = blocks_ref.shape
    weights = [
        jnp.broadcast_to(weights_ref[pl.ds(r, 1), :], (CHUNK_ROWS, LANES)) for r in range(length)
    ]
    squares, variances = [], []
    for where in chunks(rows, columns):
        values = [blocks_ref[(r, *where)].astype(jnp.float32) for r in range(length)]
        mean = total(w * v for w, v in zip(weights, values))
        deviations = [v - mean for v in values]
        variance = total(w * (d * d) for w, d in zip(weights, deviations))
        mean_ref[where] = mean
        variance_ref[where] = variance
        squares.append(to_sublanes(mean * mean))
        variances.append(to_sublanes(variance))
    squares, variances = total(squares), total(variances)
    squares = squares + pltpu.roll(squares, HALF, 1)
    variances = variances + pltpu.roll(variances, HALF, 1)
    lane = lax.broadcasted_iota(jnp.int32, squares.shape, 1)
    both = jnp.sum(jnp.where(lane < HALF, squares, variances), axis=0, keepdims=True)
    totals_ref[...] = jnp.broadcast_to(both[None], totals_ref.shape)


def update_kernel(
    element_count,
    totals_ref,
    mean_ref,
    variance_ref,
    own_ref,
    momentum_ref,
    block_ref,
    new_momentum_ref,
    scalars_ref,
):
    totals = jnp.sum(totals_ref[...], axis=0)
    lane = lax.broadcasted_iota(jnp.int32, totals.shape, 1)
    squares = jnp.sum(jnp.where(lane < HALF, totals, 0.0), axis=1, keepdims=True)
    variances = jnp.sum(jnp.where(lane < HALF, 0.0, totals), axis=1, keepdims=True)
    update_rms = jnp.sqrt(squares / element_count)
    mean_variance = variances / element_count
    which = lax.broadcasted_iota(jnp.int32, scalars_ref.shape, 0)
    scalars_ref[...] = jnp.where(which == 0, update_rms, mean_variance)
    clip_factor = clip_rms / jnp.maximum(update_rms, clip_rms)
    scale = mean_variance + epsilon
    for where in chunks(*mean_ref.shape):
        damped = clip_factor * mean_ref[where] / (1.0 + variance_ref[where] / scale)
        new_momentum = beta_outer * momentum_ref[where] + damped
        new_momentum_ref[where] = new_momentum
        outer_update = outer_rate * (damped + beta_outer * new_momentum)
        block_ref[where] = (own_ref[where].astype(jnp.float32) - outer_update).astype(jnp.bfloat16)


def store_kernel(
    params_ref,
    momentum_ref,
    scalars_ref,
    params_hbm,
    momentum_hbm,
    update_rms_hbm,
    mean_variance_hbm,
    update_rms_ref,
    mean_variance_ref,
    sems,
):
    copies = [
        pltpu.make_async_copy(momentum_ref, momentum_hbm, sems.at[0]),
        pltpu.make_async_copy(update_rms_ref, update_rms_hbm, sems.at[1]),
        pltpu.make_async_copy(mean_variance_ref, mean_variance_hbm, sems.at[2]),
    ]
    rows = params_ref.shape[0] // STORES
    for i in range(STORES):
        where = pl.ds(i * rows, rows)
        copies.append(
            pltpu.make_async_copy(params_ref.at[where], params_hbm.at[where], sems.at[3 + i])
        )
    update_rms_ref[0] = scalars_ref[0, 0]
    mean_variance_ref[0] = scalars_ref[1, 0]
    for copy in copies:
        copy.start()
    for copy in copies:
        copy.wait()


def copies_for(values, axes):
    return jnp.broadcast_to(values[None], (lax.axis_size(axes), *values.shape))


def shards(delta, counts, params, momentum):
    length = lax.axis_size(REP)
    rows, width = momentum.shape
    shape = functools.partial(jax.ShapeDtypeStruct, (rows, width))
    counts, delta, params = [
        pltpu.with_memory_space_constraint(a, pltpu.MemorySpace.HBM)
        for a in (counts, delta, params)
    ]
    blocks, own_params, weights = pl.pallas_call(
        split_kernel,
        in_specs=[HBM] * 3,
        out_specs=[VMEM] * 3,
        out_shape=[
            jax.ShapeDtypeStruct((length, rows, width), delta.dtype),
            shape(params.dtype),
            jax.ShapeDtypeStruct((length, LANES), jnp.float32),
        ],
        scratch_shapes=[pltpu.SMEM(counts.shape, counts.dtype), pltpu.SemaphoreType.DMA((length + 2,))],
        compiler_params=SMALL,
    )(counts, delta, params)
    blocks = lax.all_to_all(blocks, REP, 0, 0, tiled=True)
    first, second = SUM_STAGES
    mean, variance, totals = pl.pallas_call(
        moments_kernel,
        in_specs=[VMEM] * 2,
        out_specs=[VMEM] * 3,
        out_shape=[
            shape(jnp.float32),
            shape(jnp.float32),
            jax.ShapeDtypeStruct((lax.axis_size(first), 1, LANES), jnp.float32),
        ],
        compiler_params=SMALL,
    )(blocks, weights)
    totals = lax.all_to_all(totals, first, 0, 0, tiled=True)
    totals = copies_for(jnp.sum(totals, axis=0), second)
    totals = lax.all_to_all(totals, second, 0, 0, tiled=True)
    element_count = rows * width * length * lax.axis_size(SHARD)
    new_block, new_momentum, scalars = pl.pallas_call(
        functools.partial(update_kernel, element_count),
        in_specs=[VMEM] * 5,
        out_specs=[VMEM] * 3,
        out_shape=[
            shape(params.dtype),
            shape(jnp.float32),
            jax.ShapeDtypeStruct((2, LANES), jnp.float32),
        ],
        compiler_params=SMALL,
    )(totals, mean, variance, own_params, momentum)
    new_params = lax.all_gather(new_block, REP, axis=1, tiled=True)
    scalar = jax.ShapeDtypeStruct((1,), jnp.float32)
    new_params, new_momentum, update_rms, mean_variance = pl.pallas_call(
        store_kernel,
        in_specs=[VMEM] * 3,
        out_specs=[HBM] * 4,
        out_shape=[
            jax.ShapeDtypeStruct(params.shape, params.dtype),
            shape(jnp.float32),
            scalar,
            scalar,
        ],
        scratch_shapes=[
            pltpu.SMEM((1,), jnp.float32),
            pltpu.SMEM((1,), jnp.float32),
            pltpu.SemaphoreType.DMA((3 + STORES,)),
        ],
        compiler_params=SMALL,
    )(new_params, new_momentum, scalars)
    return (new_params, new_momentum, update_rms[0], mean_variance[0])


def solution(mesh):
    finer = Mesh(
        mesh.devices.reshape(4, 2, 2, 4, 12), ("rep_0", "rep_1", "shard_0", "shard_1", "shard_2")
    )
    in_specs = (P(REP, SHARD, None), P(), P(SHARD, None), P(SHARD, REP))
    out_specs = (P(SHARD, None), P(SHARD, REP), P(), P())
    return jax.shard_map(
        shards, mesh=finer, in_specs=in_specs, out_specs=out_specs, check_vma=False
    )
```

```python
import functools

import jax
import jax.numpy as jnp
from jax import lax
from jax.experimental import pallas as pl
from jax.experimental.pallas import tpu as pltpu
from jax.sharding import Mesh
from jax.sharding import PartitionSpec as P

REP = ("rep_0", "rep_1")
SHARD = ("shard_0", "shard_1", "shard_2")
SUM_STAGES = (("shard_1", "shard_0", "rep_0"), ("shard_2", "rep_1"))
LANES = 128
HALF = LANES // 2
STORES = 4
CHUNK_ROWS = 32

clip_rms = 0.2
beta_outer = 0.9
outer_rate = 0.7
epsilon = 1e-06

VMEM = pl.BlockSpec(memory_space=pltpu.VMEM)
HBM = pl.BlockSpec(memory_space=pltpu.MemorySpace.HBM)
SMALL = pltpu.CompilerParams(vmem_limit_bytes=8 * 1024 * 1024)


def chunks(rows, columns):
    for column in range(0, columns, LANES):
        for row in range(0, rows, CHUNK_ROWS):
            yield pl.ds(row, CHUNK_ROWS), pl.ds(column, LANES)


def total(values):
    values = list(values)
    while len(values) > 1:
        values = [sum(values[i : i + 2]) for i in range(0, len(values), 2)]
    return values[0]


def to_sublanes(values):
    return total(values[i : i + 8] for i in range(0, values.shape[0], 8))


def split_kernel(
    counts_hbm, delta_ref, params_ref, blocks_ref, own_ref, weights_ref, counts_ref, sems
):
    length, _, width = blocks_ref.shape
    mine = lax.axis_index(REP)
    copies = [
        pltpu.make_async_copy(
            delta_ref.at[0, :, pl.ds(r * width, width)], blocks_ref.at[r], sems.at[r]
        )
        for r in range(length)
    ]
    own_columns = pl.ds(pl.multiple_of(mine * width, LANES), width)
    copies.append(pltpu.make_async_copy(params_ref.at[:, own_columns], own_ref, sems.at[length]))
    counts_copy = pltpu.make_async_copy(counts_hbm, counts_ref, sems.at[length + 1])
    counts_copy.start()
    for copy in copies:
        copy.start()
    counts_copy.wait()
    row = lax.broadcasted_iota(jnp.int32, weights_ref.shape, 0)
    tokens = jnp.zeros(weights_ref.shape, jnp.float32)
    for r in range(length):
        tokens = jnp.where(row == r, counts_ref[r].astype(jnp.float32), tokens)
    all_tokens = total(counts_ref[r] for r in range(length)).astype(jnp.float32)
    weights_ref[...] = tokens / all_tokens
    for copy in copies:
        copy.wait()


def moments_kernel(blocks_ref, weights_ref, mean_ref, variance_ref, totals_ref):
    length, rows, columns = blocks_ref.shape
    weights = [
        jnp.broadcast_to(weights_ref[pl.ds(r, 1), :], (CHUNK_ROWS, LANES)) for r in range(length)
    ]
    squares, variances = [], []
    for where in chunks(rows, columns):
        values = [blocks_ref[(r, *where)].astype(jnp.float32) for r in range(length)]
        mean = total(w * v for w, v in zip(weights, values))
        deviations = [v - mean for v in values]
        variance = total(w * (d * d) for w, d in zip(weights, deviations))
        mean_ref[where] = mean
        variance_ref[where] = variance
        squares.append(to_sublanes(mean * mean))
        variances.append(to_sublanes(variance))
    squares, variances = total(squares), total(variances)
    squares = squares + pltpu.roll(squares, HALF, 1)
    variances = variances + pltpu.roll(variances, HALF, 1)
    lane = lax.broadcasted_iota(jnp.int32, squares.shape, 1)
    both = jnp.sum(jnp.where(lane < HALF, squares, variances), axis=0, keepdims=True)
    totals_ref[...] = jnp.broadcast_to(both[None], totals_ref.shape)


def update_kernel(
    element_count,
    totals_ref,
    mean_ref,
    variance_ref,
    own_ref,
    momentum_ref,
    block_ref,
    new_momentum_ref,
    scalars_ref,
):
    totals = jnp.sum(totals_ref[...], axis=0)
    lane = lax.broadcasted_iota(jnp.int32, totals.shape, 1)
    squares = jnp.sum(jnp.where(lane < HALF, totals, 0.0), axis=1, keepdims=True)
    variances = jnp.sum(jnp.where(lane < HALF, 0.0, totals), axis=1, keepdims=True)
    update_rms = jnp.sqrt(squares / element_count)
    mean_variance = variances / element_count
    which = lax.broadcasted_iota(jnp.int32, scalars_ref.shape, 0)
    scalars_ref[...] = jnp.where(which == 0, update_rms, mean_variance)
    clip_factor = clip_rms / jnp.maximum(update_rms, clip_rms)
    scale = mean_variance + epsilon
    for where in chunks(*mean_ref.shape):
        damped = clip_factor * mean_ref[where] / (1.0 + variance_ref[where] / scale)
        new_momentum = beta_outer * momentum_ref[where] + damped
        new_momentum_ref[where] = new_momentum
        outer_update = outer_rate * (damped + beta_outer * new_momentum)
        block_ref[where] = (own_ref[where].astype(jnp.float32) - outer_update).astype(jnp.bfloat16)


def store_kernel(
    params_ref,
    momentum_ref,
    scalars_ref,
    params_hbm,
    momentum_hbm,
    update_rms_hbm,
    mean_variance_hbm,
    update_rms_ref,
    mean_variance_ref,
    sems,
):
    copies = [
        pltpu.make_async_copy(momentum_ref, momentum_hbm, sems.at[0]),
        pltpu.make_async_copy(update_rms_ref, update_rms_hbm, sems.at[1]),
        pltpu.make_async_copy(mean_variance_ref, mean_variance_hbm, sems.at[2]),
    ]
    rows = params_ref.shape[0] // STORES
    for i in range(STORES):
        where = pl.ds(i * rows, rows)
        copies.append(
            pltpu.make_async_copy(params_ref.at[where], params_hbm.at[where], sems.at[3 + i])
        )
    update_rms_ref[0] = scalars_ref[0, 0]
    mean_variance_ref[0] = scalars_ref[1, 0]
    for copy in copies:
        copy.start()
    for copy in copies:
        copy.wait()


def copies_for(values, axes):
    return jnp.broadcast_to(values[None], (lax.axis_size(axes), *values.shape))


def shards(delta, counts, params, momentum):
    length = lax.axis_size(REP)
    rows, width = momentum.shape
    shape = functools.partial(jax.ShapeDtypeStruct, (rows, width))
    counts, delta, params = [
        pltpu.with_memory_space_constraint(a, pltpu.MemorySpace.HBM)
        for a in (counts, delta, params)
    ]
    blocks, own_params, weights = pl.pallas_call(
        split_kernel,
        in_specs=[HBM] * 3,
        out_specs=[VMEM] * 3,
        out_shape=[
            jax.ShapeDtypeStruct((length, rows, width), delta.dtype),
            shape(params.dtype),
            jax.ShapeDtypeStruct((length, LANES), jnp.float32),
        ],
        scratch_shapes=[pltpu.SMEM(counts.shape, counts.dtype), pltpu.SemaphoreType.DMA((length + 2,))],
        compiler_params=SMALL,
    )(counts, delta, params)
    blocks = lax.all_to_all(blocks, REP, 0, 0, tiled=True)
    first, second = SUM_STAGES
    mean, variance, totals = pl.pallas_call(
        moments_kernel,
        in_specs=[VMEM] * 2,
        out_specs=[VMEM] * 3,
        out_shape=[
            shape(jnp.float32),
            shape(jnp.float32),
            jax.ShapeDtypeStruct((lax.axis_size(first), 1, LANES), jnp.float32),
        ],
        compiler_params=SMALL,
    )(blocks, weights)
    totals = lax.all_to_all(totals, first, 0, 0, tiled=True)
    totals = copies_for(jnp.sum(totals, axis=0), second)
    totals = lax.all_to_all(totals, second, 0, 0, tiled=True)
    element_count = rows * width * length * lax.axis_size(SHARD)
    new_block, new_momentum, scalars = pl.pallas_call(
        functools.partial(update_kernel, element_count),
        in_specs=[VMEM] * 5,
        out_specs=[VMEM] * 3,
        out_shape=[
            shape(params.dtype),
            shape(jnp.float32),
            jax.ShapeDtypeStruct((2, LANES), jnp.float32),
        ],
        compiler_params=SMALL,
    )(totals, mean, variance, own_params, momentum)
    new_params = lax.all_gather(new_block, REP, axis=1, tiled=True)
    scalar = jax.ShapeDtypeStruct((1,), jnp.float32)
    new_params, new_momentum, update_rms, mean_variance = pl.pallas_call(
        store_kernel,
        in_specs=[VMEM] * 3,
        out_specs=[HBM] * 4,
        out_shape=[
            jax.ShapeDtypeStruct(params.shape, params.dtype),
            shape(jnp.float32),
            scalar,
            scalar,
        ],
        scratch_shapes=[
            pltpu.SMEM((1,), jnp.float32),
            pltpu.SMEM((1,), jnp.float32),
            pltpu.SemaphoreType.DMA((3 + STORES,)),
        ],
        compiler_params=SMALL,
    )(new_params, new_momentum, scalars)
    return (new_params, new_momentum, update_rms[0], mean_variance[0])


def solution(mesh):
    finer = Mesh(
        mesh.devices.reshape(4, 2, 2, 4, 12), ("rep_0", "rep_1", "shard_0", "shard_1", "shard_2")
    )
    in_specs = (P(REP, SHARD, None), P(), P(SHARD, None), P(SHARD, REP))
    out_specs = (P(SHARD, None), P(SHARD, REP), P(), P())
    return jax.shard_map(
        shards, mesh=finer, in_specs=in_specs, out_specs=out_specs, check_vma=False
    )
```

```python
import functools

import jax
import jax.numpy as jnp
import numpy as np
from jax import lax
from jax.experimental import pallas as pl
from jax.experimental.pallas import tpu as pltpu
from jax.sharding import Mesh
from jax.sharding import PartitionSpec as P

REP = ("rep_0", "rep_1")
SHARD = ("shard_0", "shard_1", "shard_2")
CHIPS, CORES = 4, 2
EXCHANGE_CHIPS = (0, 2, 1, 3)
GATHER_CHIPS = (0, 2, 3, 1)
LINE = ("shard_2", "rep_1")
PLANE = ("rep_0", "rep_1", "shard_0", "shard_1")
LANES = 128
HALF = LANES // 2
CHUNK_ROWS = 32

clip_rms = 0.2
beta_outer = 0.9
outer_rate = 0.7
epsilon = 1e-06

VMEM = pl.BlockSpec(memory_space=pltpu.VMEM)
HBM = pl.BlockSpec(memory_space=pltpu.MemorySpace.HBM)
SMALL = pltpu.CompilerParams(vmem_limit_bytes=8 * 1024 * 1024)


def chunks(rows, columns):
    for column in range(0, columns, LANES):
        for row in range(0, rows, CHUNK_ROWS):
            yield pl.ds(row, CHUNK_ROWS), pl.ds(column, LANES)


def ordered(chips):
    return [chip * CORES + core for chip in chips for core in range(CORES)]


def plane_groups():
    place = np.arange(CHIPS * CORES * 2 * 4).reshape(CHIPS, CORES, 2, 4)
    chips = list(np.ndindex(CHIPS, 2, 4))
    return [
        [int(place[low, core ^ (x // 2), high, x]) for low, high, x in chips]
        for core in range(CORES)
    ]


def total(values):
    values = list(values)
    while len(values) > 1:
        values = [sum(values[i : i + 2]) for i in range(0, len(values), 2)]
    return values[0]


def to_sublanes(values):
    return total(values[i : i + 8] for i in range(0, values.shape[0], 8))


def split_kernel(
    counts_hbm, delta_ref, params_ref, blocks_ref, own_ref, weights_ref, counts_ref, sems
):
    length, _, width = blocks_ref.shape
    mine = lax.axis_index(REP)
    copies = [
        pltpu.make_async_copy(
            delta_ref.at[0, :, pl.ds(r * width, width)], blocks_ref.at[i], sems.at[i]
        )
        for i, r in enumerate(ordered(EXCHANGE_CHIPS))
    ]
    own_columns = pl.ds(pl.multiple_of(mine * width, LANES), width)
    copies.append(pltpu.make_async_copy(params_ref.at[:, own_columns], own_ref, sems.at[length]))
    counts_copy = pltpu.make_async_copy(counts_hbm, counts_ref, sems.at[length + 1])
    counts_copy.start()
    for copy in copies:
        copy.start()
    counts_copy.wait()
    row = lax.broadcasted_iota(jnp.int32, weights_ref.shape, 0)
    tokens = jnp.zeros(weights_ref.shape, jnp.float32)
    for i, r in enumerate(ordered(EXCHANGE_CHIPS)):
        tokens = jnp.where(row == i, counts_ref[r].astype(jnp.float32), tokens)
    all_tokens = total(counts_ref[r] for r in range(length)).astype(jnp.float32)
    weights_ref[...] = tokens / all_tokens
    for copy in copies:
        copy.wait()


def moments_kernel(blocks_ref, weights_ref, mean_ref, variance_ref, totals_ref):
    length, rows, columns = blocks_ref.shape
    weights = [
        jnp.broadcast_to(weights_ref[pl.ds(r, 1), :], (CHUNK_ROWS, LANES)) for r in range(length)
    ]
    squares, variances = [], []
    for where in chunks(rows, columns):
        values = [blocks_ref[(r, *where)].astype(jnp.float32) for r in range(length)]
        mean = total(w * v for w, v in zip(weights, values))
        deviations = [v - mean for v in values]
        variance = total(w * (d * d) for w, d in zip(weights, deviations))
        mean_ref[where] = mean
        variance_ref[where] = variance
        squares.append(to_sublanes(mean * mean))
        variances.append(to_sublanes(variance))
    squares, variances = total(squares), total(variances)
    squares = squares + pltpu.roll(squares, HALF, 1)
    variances = variances + pltpu.roll(variances, HALF, 1)
    lane = lax.broadcasted_iota(jnp.int32, squares.shape, 1)
    both = jnp.sum(jnp.where(lane < HALF, squares, variances), axis=0, keepdims=True)
    totals_ref[...] = jnp.broadcast_to(both[None], totals_ref.shape)


def update_kernel(
    element_count,
    totals_ref,
    mean_ref,
    variance_ref,
    own_ref,
    momentum_ref,
    block_ref,
    new_momentum_ref,
    scalars_ref,
):
    totals = jnp.sum(totals_ref[...], axis=0)
    lane = lax.broadcasted_iota(jnp.int32, totals.shape, 1)
    squares = jnp.sum(jnp.where(lane < HALF, totals, 0.0), axis=1, keepdims=True)
    variances = jnp.sum(jnp.where(lane < HALF, 0.0, totals), axis=1, keepdims=True)
    update_rms = jnp.sqrt(squares / element_count)
    mean_variance = variances / element_count
    which = lax.broadcasted_iota(jnp.int32, scalars_ref.shape, 0)
    scalars_ref[...] = jnp.where(which == 0, update_rms, mean_variance)
    clip_factor = clip_rms / jnp.maximum(update_rms, clip_rms)
    scale = mean_variance + epsilon
    for where in chunks(*mean_ref.shape):
        damped = clip_factor * mean_ref[where] / (1.0 + variance_ref[where] / scale)
        new_momentum = beta_outer * momentum_ref[where] + damped
        new_momentum_ref[where] = new_momentum
        outer_update = outer_rate * (damped + beta_outer * new_momentum)
        block_ref[where] = (own_ref[where].astype(jnp.float32) - outer_update).astype(jnp.bfloat16)


def store_kernel(
    params_ref,
    momentum_ref,
    scalars_ref,
    params_hbm,
    momentum_hbm,
    update_rms_hbm,
    mean_variance_hbm,
    update_rms_ref,
    mean_variance_ref,
    sems,
):
    copies = [
        pltpu.make_async_copy(momentum_ref, momentum_hbm, sems.at[0]),
        pltpu.make_async_copy(update_rms_ref, update_rms_hbm, sems.at[1]),
        pltpu.make_async_copy(mean_variance_ref, mean_variance_hbm, sems.at[2]),
    ]
    width = params_ref.shape[1] // CHIPS
    for i, chip in enumerate(GATHER_CHIPS):
        here, there = pl.ds(i * width, width), pl.ds(chip * width, width)
        copies.append(
            pltpu.make_async_copy(params_ref.at[:, here], params_hbm.at[:, there], sems.at[3 + i])
        )
    update_rms_ref[0] = scalars_ref[0, 0]
    mean_variance_ref[0] = scalars_ref[1, 0]
    for copy in copies:
        copy.start()
    for copy in copies:
        copy.wait()


def exchanged(blocks, axes, groups=None):
    return lax.all_to_all(blocks, axes, 0, 0, axis_index_groups=groups, tiled=True)


def shards(delta, counts, params, momentum):
    length = lax.axis_size(REP)
    rows, width = momentum.shape
    shape = functools.partial(jax.ShapeDtypeStruct, (rows, width))
    counts, delta, params = [
        pltpu.with_memory_space_constraint(a, pltpu.MemorySpace.HBM)
        for a in (counts, delta, params)
    ]
    blocks, own_params, weights = pl.pallas_call(
        split_kernel,
        in_specs=[HBM] * 3,
        out_specs=[VMEM] * 3,
        out_shape=[
            jax.ShapeDtypeStruct((length, rows, width), delta.dtype),
            shape(params.dtype),
            jax.ShapeDtypeStruct((length, LANES), jnp.float32),
        ],
        scratch_shapes=[pltpu.SMEM(counts.shape, counts.dtype), pltpu.SemaphoreType.DMA((length + 2,))],
        compiler_params=SMALL,
    )(counts, delta, params)
    blocks = exchanged(blocks, REP, [ordered(EXCHANGE_CHIPS)])
    mean, variance, totals = pl.pallas_call(
        moments_kernel,
        in_specs=[VMEM] * 2,
        out_specs=[VMEM] * 3,
        out_shape=[
            shape(jnp.float32),
            shape(jnp.float32),
            jax.ShapeDtypeStruct((lax.axis_size(LINE), 1, LANES), jnp.float32),
        ],
        compiler_params=SMALL,
    )(blocks, weights)
    line_totals = jnp.sum(exchanged(totals, LINE), axis=0)
    groups = plane_groups()
    totals = jnp.broadcast_to(line_totals[None], (len(groups[0]), *line_totals.shape))
    totals = exchanged(totals, PLANE, groups)
    element_count = rows * width * length * lax.axis_size(SHARD)
    new_block, new_momentum, scalars = pl.pallas_call(
        functools.partial(update_kernel, element_count),
        in_specs=[VMEM] * 5,
        out_specs=[VMEM] * 3,
        out_shape=[
            shape(params.dtype),
            shape(jnp.float32),
            jax.ShapeDtypeStruct((2, LANES), jnp.float32),
        ],
        compiler_params=SMALL,
    )(totals, mean, variance, own_params, momentum)
    new_params = lax.all_gather(
        new_block, REP, axis_index_groups=[ordered(GATHER_CHIPS)], axis=1, tiled=True
    )
    scalar = jax.ShapeDtypeStruct((1,), jnp.float32)
    new_params, new_momentum, update_rms, mean_variance = pl.pallas_call(
        store_kernel,
        in_specs=[VMEM] * 3,
        out_specs=[HBM] * 4,
        out_shape=[
            jax.ShapeDtypeStruct(params.shape, params.dtype),
            shape(jnp.float32),
            scalar,
            scalar,
        ],
        scratch_shapes=[
            pltpu.SMEM((1,), jnp.float32),
            pltpu.SMEM((1,), jnp.float32),
            pltpu.SemaphoreType.DMA((3 + CHIPS,)),
        ],
        compiler_params=SMALL,
    )(new_params, new_momentum, scalars)
    return (new_params, new_momentum, update_rms[0], mean_variance[0])


def solution(mesh):
    finer = Mesh(
        mesh.devices.reshape(4, 2, 2, 4, 12), ("rep_0", "rep_1", "shard_0", "shard_1", "shard_2")
    )
    in_specs = (P(REP, SHARD, None), P(), P(SHARD, None), P(SHARD, REP))
    out_specs = (P(SHARD, None), P(SHARD, REP), P(), P())
    return jax.shard_map(
        shards, mesh=finer, in_specs=in_specs, out_specs=out_specs, check_vma=False
    )
```

```python
import functools

import jax
import jax.numpy as jnp
import numpy as np
from jax import lax
from jax.experimental import pallas as pl
from jax.experimental.pallas import tpu as pltpu
from jax.sharding import Mesh
from jax.sharding import PartitionSpec as P

REP = ("rep_0", "rep_1")
SHARD = ("shard_0", "shard_1", "shard_2")
CHIPS, CORES = 4, 2
EXCHANGE_CHIPS = (2, 0, 3, 1)
GATHER_CHIPS = (1, 0, 2, 3)
LINE = ("shard_2", "rep_1")
PLANE = ("rep_0", "rep_1", "shard_0", "shard_1")
LINE_CHIPS, LINE_START = 12, 8
PLANE_START = (2, 6)
LANES = 128
HALF = LANES // 2
CHUNK_ROWS = 32

clip_rms = 0.2
beta_outer = 0.9
outer_rate = 0.7
epsilon = 1e-06

VMEM = pl.BlockSpec(memory_space=pltpu.VMEM)
HBM = pl.BlockSpec(memory_space=pltpu.MemorySpace.HBM)
SMALL = pltpu.CompilerParams(vmem_limit_bytes=8 * 1024 * 1024)


def chunks(rows, columns):
    for column in range(0, columns, LANES):
        for row in range(0, rows, CHUNK_ROWS):
            yield pl.ds(row, CHUNK_ROWS), pl.ds(column, LANES)


def ordered(chips):
    return [chip * CORES + core for chip in chips for core in range(CORES)]


def ring_distance(a, b, length):
    return min((a - b) % length, (b - a) % length)


def line_group():
    order = sorted(range(LINE_CHIPS), key=lambda z: ring_distance(z, LINE_START, LINE_CHIPS))
    return [z * CORES + core for z in order for core in (1, 0)]


def plane_groups():
    highs, xs = 2, 4
    place = np.arange(CHIPS * CORES * highs * xs).reshape(CHIPS, CORES, highs, xs)

    def distance(chip):
        low, high, x = chip
        start_x, start_y = PLANE_START
        y = high * CHIPS + low
        return ring_distance(x, start_x, xs) + ring_distance(y, start_y, highs * CHIPS)

    chips = sorted(np.ndindex(CHIPS, highs, xs), key=distance)
    return [
        [int(place[low, core ^ (x // 2), high, x]) for low, high, x in chips]
        for core in range(CORES)
    ]


def total(values):
    values = list(values)
    while len(values) > 1:
        values = [sum(values[i : i + 2]) for i in range(0, len(values), 2)]
    return values[0]


def to_sublanes(values):
    return total(values[i : i + 8] for i in range(0, values.shape[0], 8))


def split_kernel(
    counts_hbm, delta_ref, params_ref, blocks_ref, own_ref, weights_ref, counts_ref, sems
):
    length, _, width = blocks_ref.shape
    mine = lax.axis_index(REP)
    copies = [
        pltpu.make_async_copy(
            delta_ref.at[0, :, pl.ds(r * width, width)], blocks_ref.at[i], sems.at[i]
        )
        for i, r in enumerate(ordered(EXCHANGE_CHIPS))
    ]
    own_columns = pl.ds(pl.multiple_of(mine * width, LANES), width)
    copies.append(pltpu.make_async_copy(params_ref.at[:, own_columns], own_ref, sems.at[length]))
    counts_copy = pltpu.make_async_copy(counts_hbm, counts_ref, sems.at[length + 1])
    counts_copy.start()
    for copy in copies:
        copy.start()
    counts_copy.wait()
    row = lax.broadcasted_iota(jnp.int32, weights_ref.shape, 0)
    tokens = jnp.zeros(weights_ref.shape, jnp.float32)
    for i, r in enumerate(ordered(EXCHANGE_CHIPS)):
        tokens = jnp.where(row == i, counts_ref[r].astype(jnp.float32), tokens)
    all_tokens = total(counts_ref[r] for r in range(length)).astype(jnp.float32)
    weights_ref[...] = tokens / all_tokens
    for copy in copies:
        copy.wait()


def moments_kernel(blocks_ref, weights_ref, mean_ref, variance_ref, totals_ref):
    length, rows, columns = blocks_ref.shape
    weights = [
        jnp.broadcast_to(weights_ref[pl.ds(r, 1), :], (CHUNK_ROWS, LANES)) for r in range(length)
    ]
    squares, variances = [], []
    for where in chunks(rows, columns):
        values = [blocks_ref[(r, *where)].astype(jnp.float32) for r in range(length)]
        mean = total(w * v for w, v in zip(weights, values))
        deviations = [v - mean for v in values]
        variance = total(w * (d * d) for w, d in zip(weights, deviations))
        mean_ref[where] = mean
        variance_ref[where] = variance
        squares.append(to_sublanes(mean * mean))
        variances.append(to_sublanes(variance))
    squares, variances = total(squares), total(variances)
    squares = squares + pltpu.roll(squares, HALF, 1)
    variances = variances + pltpu.roll(variances, HALF, 1)
    lane = lax.broadcasted_iota(jnp.int32, squares.shape, 1)
    both = jnp.sum(jnp.where(lane < HALF, squares, variances), axis=0, keepdims=True)
    totals_ref[...] = jnp.broadcast_to(both[None], totals_ref.shape)


def update_kernel(
    element_count,
    totals_ref,
    mean_ref,
    variance_ref,
    own_ref,
    momentum_ref,
    block_ref,
    new_momentum_ref,
    scalars_ref,
):
    totals = jnp.sum(totals_ref[...], axis=0)
    lane = lax.broadcasted_iota(jnp.int32, totals.shape, 1)
    squares = jnp.sum(jnp.where(lane < HALF, totals, 0.0), axis=1, keepdims=True)
    variances = jnp.sum(jnp.where(lane < HALF, 0.0, totals), axis=1, keepdims=True)
    update_rms = jnp.sqrt(squares / element_count)
    mean_variance = variances / element_count
    which = lax.broadcasted_iota(jnp.int32, scalars_ref.shape, 0)
    scalars_ref[...] = jnp.where(which == 0, update_rms, mean_variance)
    clip_factor = clip_rms / jnp.maximum(update_rms, clip_rms)
    scale = mean_variance + epsilon
    for where in chunks(*mean_ref.shape):
        damped = clip_factor * mean_ref[where] / (1.0 + variance_ref[where] / scale)
        new_momentum = beta_outer * momentum_ref[where] + damped
        new_momentum_ref[where] = new_momentum
        outer_update = outer_rate * (damped + beta_outer * new_momentum)
        block_ref[where] = (own_ref[where].astype(jnp.float32) - outer_update).astype(jnp.bfloat16)


def store_kernel(
    params_ref,
    momentum_ref,
    scalars_ref,
    params_hbm,
    momentum_hbm,
    update_rms_hbm,
    mean_variance_hbm,
    update_rms_ref,
    mean_variance_ref,
    sems,
):
    copies = [
        pltpu.make_async_copy(momentum_ref, momentum_hbm, sems.at[0]),
        pltpu.make_async_copy(update_rms_ref, update_rms_hbm, sems.at[1]),
        pltpu.make_async_copy(mean_variance_ref, mean_variance_hbm, sems.at[2]),
    ]
    width = params_ref.shape[1] // CHIPS
    for i, chip in enumerate(GATHER_CHIPS):
        here, there = pl.ds(i * width, width), pl.ds(chip * width, width)
        copies.append(
            pltpu.make_async_copy(params_ref.at[:, here], params_hbm.at[:, there], sems.at[3 + i])
        )
    update_rms_ref[0] = scalars_ref[0, 0]
    mean_variance_ref[0] = scalars_ref[1, 0]
    for copy in copies:
        copy.start()
    for copy in copies:
        copy.wait()


def exchanged(blocks, axes, groups=None):
    return lax.all_to_all(blocks, axes, 0, 0, axis_index_groups=groups, tiled=True)


def shards(delta, counts, params, momentum):
    length = lax.axis_size(REP)
    rows, width = momentum.shape
    shape = functools.partial(jax.ShapeDtypeStruct, (rows, width))
    counts, delta, params = [
        pltpu.with_memory_space_constraint(a, pltpu.MemorySpace.HBM)
        for a in (counts, delta, params)
    ]
    blocks, own_params, weights = pl.pallas_call(
        split_kernel,
        in_specs=[HBM] * 3,
        out_specs=[VMEM] * 3,
        out_shape=[
            jax.ShapeDtypeStruct((length, rows, width), delta.dtype),
            shape(params.dtype),
            jax.ShapeDtypeStruct((length, LANES), jnp.float32),
        ],
        scratch_shapes=[pltpu.SMEM(counts.shape, counts.dtype), pltpu.SemaphoreType.DMA((length + 2,))],
        compiler_params=SMALL,
    )(counts, delta, params)
    blocks = exchanged(blocks, REP, [ordered(EXCHANGE_CHIPS)])
    mean, variance, totals = pl.pallas_call(
        moments_kernel,
        in_specs=[VMEM] * 2,
        out_specs=[VMEM] * 3,
        out_shape=[
            shape(jnp.float32),
            shape(jnp.float32),
            jax.ShapeDtypeStruct((lax.axis_size(LINE), 1, LANES), jnp.float32),
        ],
        compiler_params=SMALL,
    )(blocks, weights)
    line_totals = jnp.sum(exchanged(totals, LINE, [line_group()]), axis=0)
    groups = plane_groups()
    totals = jnp.broadcast_to(line_totals[None], (len(groups[0]), *line_totals.shape))
    totals = exchanged(totals, PLANE, groups)
    element_count = rows * width * length * lax.axis_size(SHARD)
    new_block, new_momentum, scalars = pl.pallas_call(
        functools.partial(update_kernel, element_count),
        in_specs=[VMEM] * 5,
        out_specs=[VMEM] * 3,
        out_shape=[
            shape(params.dtype),
            shape(jnp.float32),
            jax.ShapeDtypeStruct((2, LANES), jnp.float32),
        ],
        compiler_params=SMALL,
    )(totals, mean, variance, own_params, momentum)
    new_params = lax.all_gather(
        new_block, REP, axis_index_groups=[ordered(GATHER_CHIPS)], axis=1, tiled=True
    )
    scalar = jax.ShapeDtypeStruct((1,), jnp.float32)
    new_params, new_momentum, update_rms, mean_variance = pl.pallas_call(
        store_kernel,
        in_specs=[VMEM] * 3,
        out_specs=[HBM] * 4,
        out_shape=[
            jax.ShapeDtypeStruct(params.shape, params.dtype),
            shape(jnp.float32),
            scalar,
            scalar,
        ],
        scratch_shapes=[
            pltpu.SMEM((1,), jnp.float32),
            pltpu.SMEM((1,), jnp.float32),
            pltpu.SemaphoreType.DMA((3 + CHIPS,)),
        ],
        compiler_params=SMALL,
    )(new_params, new_momentum, scalars)
    return (new_params, new_momentum, update_rms[0], mean_variance[0])


def solution(mesh):
    finer = Mesh(
        mesh.devices.reshape(4, 2, 2, 4, 12), ("rep_0", "rep_1", "shard_0", "shard_1", "shard_2")
    )
    in_specs = (P(REP, SHARD, None), P(), P(SHARD, None), P(SHARD, REP))
    out_specs = (P(SHARD, None), P(SHARD, REP), P(), P())
    return jax.shard_map(
        shards, mesh=finer, in_specs=in_specs, out_specs=out_specs, check_vma=False
    )
```

```python
import functools

import jax
import jax.numpy as jnp
import numpy as np
from jax import lax
from jax.experimental import pallas as pl
from jax.experimental.pallas import tpu as pltpu
from jax.sharding import Mesh
from jax.sharding import PartitionSpec as P

REP = ("rep_0", "rep_1")
SHARD = ("shard_0", "shard_1", "shard_2")
CHIPS, CORES = 4, 2
EXCHANGE_CHIPS = (2, 0, 3, 1)
GATHER_CHIPS = (1, 0, 2, 3)
LINE = ("shard_2", "rep_1")
PLANE = ("rep_0", "rep_1", "shard_0", "shard_1")
LINE_CHIPS, LINE_START = 12, 8
PLANE_START = (2, 6)
LANES = 128
HALF = LANES // 2
CHUNK_ROWS = 32

clip_rms = 0.2
beta_outer = 0.9
outer_rate = 0.7
epsilon = 1e-06

VMEM = pl.BlockSpec(memory_space=pltpu.VMEM)
HBM = pl.BlockSpec(memory_space=pltpu.MemorySpace.HBM)
SMALL = pltpu.CompilerParams(vmem_limit_bytes=8 * 1024 * 1024)


def chunks(rows, columns):
    for column in range(0, columns, LANES):
        for row in range(0, rows, CHUNK_ROWS):
            yield pl.ds(row, CHUNK_ROWS), pl.ds(column, LANES)


def ordered(chips, cores=(1, 0)):
    return [chip * CORES + core for chip in chips for core in cores]


def ring_distance(a, b, length):
    return min((a - b) % length, (b - a) % length)


def line_group():
    order = sorted(range(LINE_CHIPS), key=lambda z: ring_distance(z, LINE_START, LINE_CHIPS))
    return ordered(order)


def plane_groups():
    highs, xs = 2, 4
    place = np.arange(CHIPS * CORES * highs * xs).reshape(CHIPS, CORES, highs, xs)

    def distance(chip):
        low, high, x = chip
        start_x, start_y = PLANE_START
        y = high * CHIPS + low
        return ring_distance(x, start_x, xs) + ring_distance(y, start_y, highs * CHIPS)

    chips = sorted(np.ndindex(CHIPS, highs, xs), key=distance)
    return [
        [int(place[low, core ^ (x // 2), high, x]) for low, high, x in chips]
        for core in range(CORES)
    ]


def total(values):
    values = list(values)
    while len(values) > 1:
        values = [sum(values[i : i + 2]) for i in range(0, len(values), 2)]
    return values[0]


def to_sublanes(values):
    return total(values[i : i + 8] for i in range(0, values.shape[0], 8))


def split_kernel(
    counts_hbm, delta_ref, params_ref, blocks_ref, own_ref, weights_ref, counts_ref, sems
):
    length, _, width = blocks_ref.shape
    mine = lax.axis_index(REP)
    copies = [
        pltpu.make_async_copy(
            delta_ref.at[0, :, pl.ds(r * width, width)], blocks_ref.at[i], sems.at[i]
        )
        for i, r in enumerate(ordered(EXCHANGE_CHIPS))
    ]
    own_columns = pl.ds(pl.multiple_of(mine * width, LANES), width)
    copies.append(pltpu.make_async_copy(params_ref.at[:, own_columns], own_ref, sems.at[length]))
    counts_copy = pltpu.make_async_copy(counts_hbm, counts_ref, sems.at[length + 1])
    counts_copy.start()
    for copy in copies:
        copy.start()
    counts_copy.wait()
    row = lax.broadcasted_iota(jnp.int32, weights_ref.shape, 0)
    tokens = jnp.zeros(weights_ref.shape, jnp.float32)
    for i, r in enumerate(ordered(EXCHANGE_CHIPS)):
        tokens = jnp.where(row == i, counts_ref[r].astype(jnp.float32), tokens)
    all_tokens = total(counts_ref[r] for r in range(length)).astype(jnp.float32)
    weights_ref[...] = tokens / all_tokens
    for copy in copies:
        copy.wait()


def moments_kernel(blocks_ref, weights_ref, mean_ref, variance_ref, totals_ref):
    length, rows, columns = blocks_ref.shape
    weights = [
        jnp.broadcast_to(weights_ref[pl.ds(r, 1), :], (CHUNK_ROWS, LANES)) for r in range(length)
    ]
    squares, variances = [], []
    for where in chunks(rows, columns):
        values = [blocks_ref[(r, *where)].astype(jnp.float32) for r in range(length)]
        mean = total(w * v for w, v in zip(weights, values))
        deviations = [v - mean for v in values]
        variance = total(w * (d * d) for w, d in zip(weights, deviations))
        mean_ref[where] = mean
        variance_ref[where] = variance
        squares.append(to_sublanes(mean * mean))
        variances.append(to_sublanes(variance))
    squares, variances = total(squares), total(variances)
    squares = squares + pltpu.roll(squares, HALF, 1)
    variances = variances + pltpu.roll(variances, HALF, 1)
    lane = lax.broadcasted_iota(jnp.int32, squares.shape, 1)
    both = jnp.sum(jnp.where(lane < HALF, squares, variances), axis=0, keepdims=True)
    totals_ref[...] = jnp.broadcast_to(both[None], totals_ref.shape)


def update_kernel(
    element_count,
    totals_ref,
    mean_ref,
    variance_ref,
    own_ref,
    momentum_ref,
    block_ref,
    new_momentum_ref,
    scalars_ref,
):
    totals = jnp.sum(totals_ref[...], axis=0)
    lane = lax.broadcasted_iota(jnp.int32, totals.shape, 1)
    squares = jnp.sum(jnp.where(lane < HALF, totals, 0.0), axis=1, keepdims=True)
    variances = jnp.sum(jnp.where(lane < HALF, 0.0, totals), axis=1, keepdims=True)
    update_rms = jnp.sqrt(squares / element_count)
    mean_variance = variances / element_count
    which = lax.broadcasted_iota(jnp.int32, scalars_ref.shape, 0)
    scalars_ref[...] = jnp.where(which == 0, update_rms, mean_variance)
    clip_factor = clip_rms / jnp.maximum(update_rms, clip_rms)
    scale = mean_variance + epsilon
    for where in chunks(*mean_ref.shape):
        damped = clip_factor * mean_ref[where] / (1.0 + variance_ref[where] / scale)
        new_momentum = beta_outer * momentum_ref[where] + damped
        new_momentum_ref[where] = new_momentum
        outer_update = outer_rate * (damped + beta_outer * new_momentum)
        block_ref[where] = (own_ref[where].astype(jnp.float32) - outer_update).astype(jnp.bfloat16)


def store_kernel(
    params_ref,
    momentum_ref,
    scalars_ref,
    params_hbm,
    momentum_hbm,
    update_rms_hbm,
    mean_variance_hbm,
    update_rms_ref,
    mean_variance_ref,
    sems,
):
    copies = [
        pltpu.make_async_copy(momentum_ref, momentum_hbm, sems.at[0]),
        pltpu.make_async_copy(update_rms_ref, update_rms_hbm, sems.at[1]),
        pltpu.make_async_copy(mean_variance_ref, mean_variance_hbm, sems.at[2]),
    ]
    width = params_ref.shape[1] // CHIPS
    for i, chip in enumerate(GATHER_CHIPS):
        here, there = pl.ds(i * width, width), pl.ds(chip * width, width)
        copies.append(
            pltpu.make_async_copy(params_ref.at[:, here], params_hbm.at[:, there], sems.at[3 + i])
        )
    update_rms_ref[0] = scalars_ref[0, 0]
    mean_variance_ref[0] = scalars_ref[1, 0]
    for copy in copies:
        copy.start()
    for copy in copies:
        copy.wait()


def exchanged(blocks, axes, groups=None):
    return lax.all_to_all(blocks, axes, 0, 0, axis_index_groups=groups, tiled=True)


def shards(delta, counts, params, momentum):
    length = lax.axis_size(REP)
    rows, width = momentum.shape
    shape = functools.partial(jax.ShapeDtypeStruct, (rows, width))
    counts, delta, params = [
        pltpu.with_memory_space_constraint(a, pltpu.MemorySpace.HBM)
        for a in (counts, delta, params)
    ]
    blocks, own_params, weights = pl.pallas_call(
        split_kernel,
        in_specs=[HBM] * 3,
        out_specs=[VMEM] * 3,
        out_shape=[
            jax.ShapeDtypeStruct((length, rows, width), delta.dtype),
            shape(params.dtype),
            jax.ShapeDtypeStruct((length, LANES), jnp.float32),
        ],
        scratch_shapes=[pltpu.SMEM(counts.shape, counts.dtype), pltpu.SemaphoreType.DMA((length + 2,))],
        compiler_params=SMALL,
    )(counts, delta, params)
    blocks = exchanged(blocks, REP, [ordered(EXCHANGE_CHIPS)])
    mean, variance, totals = pl.pallas_call(
        moments_kernel,
        in_specs=[VMEM] * 2,
        out_specs=[VMEM] * 3,
        out_shape=[
            shape(jnp.float32),
            shape(jnp.float32),
            jax.ShapeDtypeStruct((lax.axis_size(LINE), 1, LANES), jnp.float32),
        ],
        compiler_params=SMALL,
    )(blocks, weights)
    line_totals = jnp.sum(exchanged(totals, LINE, [line_group()]), axis=0)
    groups = plane_groups()
    totals = jnp.broadcast_to(line_totals[None], (len(groups[0]), *line_totals.shape))
    totals = exchanged(totals, PLANE, groups)
    element_count = rows * width * length * lax.axis_size(SHARD)
    new_block, new_momentum, scalars = pl.pallas_call(
        functools.partial(update_kernel, element_count),
        in_specs=[VMEM] * 5,
        out_specs=[VMEM] * 3,
        out_shape=[
            shape(params.dtype),
            shape(jnp.float32),
            jax.ShapeDtypeStruct((2, LANES), jnp.float32),
        ],
        compiler_params=SMALL,
    )(totals, mean, variance, own_params, momentum)
    new_params = lax.all_gather(
        new_block, REP, axis_index_groups=[ordered(GATHER_CHIPS, range(CORES))], axis=1, tiled=True
    )
    scalar = jax.ShapeDtypeStruct((1,), jnp.float32)
    new_params, new_momentum, update_rms, mean_variance = pl.pallas_call(
        store_kernel,
        in_specs=[VMEM] * 3,
        out_specs=[HBM] * 4,
        out_shape=[
            jax.ShapeDtypeStruct(params.shape, params.dtype),
            shape(jnp.float32),
            scalar,
            scalar,
        ],
        scratch_shapes=[
            pltpu.SMEM((1,), jnp.float32),
            pltpu.SMEM((1,), jnp.float32),
            pltpu.SemaphoreType.DMA((3 + CHIPS,)),
        ],
        compiler_params=SMALL,
    )(new_params, new_momentum, scalars)
    return (new_params, new_momentum, update_rms[0], mean_variance[0])


def solution(mesh):
    finer = Mesh(
        mesh.devices.reshape(4, 2, 2, 4, 12), ("rep_0", "rep_1", "shard_0", "shard_1", "shard_2")
    )
    in_specs = (P(REP, SHARD, None), P(), P(SHARD, None), P(SHARD, REP))
    out_specs = (P(SHARD, None), P(SHARD, REP), P(), P())
    return jax.shard_map(
        shards, mesh=finer, in_specs=in_specs, out_specs=out_specs, check_vma=False
    )
```

```python
import functools

import jax
import jax.numpy as jnp
import numpy as np
from jax import lax
from jax.experimental import pallas as pl
from jax.experimental.pallas import tpu as pltpu
from jax.sharding import Mesh
from jax.sharding import PartitionSpec as P

REP = ("rep_0", "rep_1")
SHARD = ("shard_0", "shard_1", "shard_2")
CHIPS, CORES = 4, 2
EXCHANGE_CHIPS = (2, 0, 3, 1)
GATHER_CHIPS = (1, 0, 2, 3)
LINE = ("shard_2", "rep_1")
PLANE = ("rep_0", "rep_1", "shard_0", "shard_1")
LINE_CHIPS, LINE_START = 12, 8
PLANE_START = (2, 6)
LANES = 128
HALF = LANES // 2
CHUNK_ROWS = 32

clip_rms = 0.2
beta_outer = 0.9
outer_rate = 0.7
epsilon = 1e-06

VMEM = pl.BlockSpec(memory_space=pltpu.VMEM)
HBM = pl.BlockSpec(memory_space=pltpu.MemorySpace.HBM)
SMALL = pltpu.CompilerParams(vmem_limit_bytes=8 * 1024 * 1024)


def chunks(rows, columns):
    for column in range(0, columns, LANES):
        for row in range(0, rows, CHUNK_ROWS):
            yield pl.ds(row, CHUNK_ROWS), pl.ds(column, LANES)


def ordered(chips):
    return [chip * CORES + core for chip in chips for core in (1, 0)]


def ring_distance(a, b, length):
    return min((a - b) % length, (b - a) % length)


def line_group():
    order = sorted(range(LINE_CHIPS), key=lambda z: ring_distance(z, LINE_START, LINE_CHIPS))
    return ordered(order)


def plane_groups():
    highs, xs = 2, 4
    place = np.arange(CHIPS * CORES * highs * xs).reshape(CHIPS, CORES, highs, xs)

    def distance(chip):
        low, high, x = chip
        start_x, start_y = PLANE_START
        y = high * CHIPS + low
        return ring_distance(x, start_x, xs) + ring_distance(y, start_y, highs * CHIPS)

    chips = sorted(np.ndindex(CHIPS, highs, xs), key=distance)
    return [
        [int(place[low, core ^ (x // 2), high, x]) for low, high, x in chips]
        for core in range(CORES)
    ]


def total(values):
    values = list(values)
    while len(values) > 1:
        values = [sum(values[i : i + 2]) for i in range(0, len(values), 2)]
    return values[0]


def to_sublanes(values):
    return total(values[i : i + 8] for i in range(0, values.shape[0], 8))


def split_kernel(
    counts_hbm, delta_ref, params_ref, blocks_ref, own_ref, weights_ref, counts_ref, sems
):
    length, _, width = blocks_ref.shape
    mine = lax.axis_index(REP)
    copies = [
        pltpu.make_async_copy(
            delta_ref.at[0, :, pl.ds(r * width, width)], blocks_ref.at[i], sems.at[i]
        )
        for i, r in enumerate(ordered(EXCHANGE_CHIPS))
    ]
    own_columns = pl.ds(pl.multiple_of(mine * width, LANES), width)
    copies.append(pltpu.make_async_copy(params_ref.at[:, own_columns], own_ref, sems.at[length]))
    counts_copy = pltpu.make_async_copy(counts_hbm, counts_ref, sems.at[length + 1])
    counts_copy.start()
    for copy in copies:
        copy.start()
    counts_copy.wait()
    row = lax.broadcasted_iota(jnp.int32, weights_ref.shape, 0)
    tokens = jnp.zeros(weights_ref.shape, jnp.float32)
    for i, r in enumerate(ordered(EXCHANGE_CHIPS)):
        tokens = jnp.where(row == i, counts_ref[r].astype(jnp.float32), tokens)
    all_tokens = total(counts_ref[r] for r in range(length)).astype(jnp.float32)
    weights_ref[...] = tokens / all_tokens
    for copy in copies:
        copy.wait()


def moments_kernel(blocks_ref, weights_ref, mean_ref, variance_ref, totals_ref):
    length, rows, columns = blocks_ref.shape
    weights = [
        jnp.broadcast_to(weights_ref[pl.ds(r, 1), :], (CHUNK_ROWS, LANES)) for r in range(length)
    ]
    squares, variances = [], []
    for where in chunks(rows, columns):
        values = [blocks_ref[(r, *where)].astype(jnp.float32) for r in range(length)]
        mean = total(w * v for w, v in zip(weights, values))
        deviations = [v - mean for v in values]
        variance = total(w * (d * d) for w, d in zip(weights, deviations))
        mean_ref[where] = mean
        variance_ref[where] = variance
        squares.append(to_sublanes(mean * mean))
        variances.append(to_sublanes(variance))
    squares, variances = total(squares), total(variances)
    squares = squares + pltpu.roll(squares, HALF, 1)
    variances = variances + pltpu.roll(variances, HALF, 1)
    lane = lax.broadcasted_iota(jnp.int32, squares.shape, 1)
    both = jnp.sum(jnp.where(lane < HALF, squares, variances), axis=0, keepdims=True)
    totals_ref[...] = jnp.broadcast_to(both[None], totals_ref.shape)


def update_kernel(
    element_count,
    totals_ref,
    mean_ref,
    variance_ref,
    own_ref,
    momentum_ref,
    block_ref,
    new_momentum_ref,
    scalars_ref,
):
    totals = jnp.sum(totals_ref[...], axis=0)
    lane = lax.broadcasted_iota(jnp.int32, totals.shape, 1)
    squares = jnp.sum(jnp.where(lane < HALF, totals, 0.0), axis=1, keepdims=True)
    variances = jnp.sum(jnp.where(lane < HALF, 0.0, totals), axis=1, keepdims=True)
    update_rms = jnp.sqrt(squares / element_count)
    mean_variance = variances / element_count
    which = lax.broadcasted_iota(jnp.int32, scalars_ref.shape, 0)
    scalars_ref[...] = jnp.where(which == 0, update_rms, mean_variance)
    clip_factor = clip_rms / jnp.maximum(update_rms, clip_rms)
    scale = mean_variance + epsilon
    for where in chunks(*mean_ref.shape):
        damped = clip_factor * mean_ref[where] / (1.0 + variance_ref[where] / scale)
        new_momentum = beta_outer * momentum_ref[where] + damped
        new_momentum_ref[where] = new_momentum
        outer_update = outer_rate * (damped + beta_outer * new_momentum)
        block_ref[where] = (own_ref[where].astype(jnp.float32) - outer_update).astype(jnp.bfloat16)


def store_kernel(
    params_ref,
    momentum_ref,
    scalars_ref,
    params_hbm,
    momentum_hbm,
    update_rms_hbm,
    mean_variance_hbm,
    update_rms_ref,
    mean_variance_ref,
    sems,
):
    copies = [
        pltpu.make_async_copy(momentum_ref, momentum_hbm, sems.at[0]),
        pltpu.make_async_copy(update_rms_ref, update_rms_hbm, sems.at[1]),
        pltpu.make_async_copy(mean_variance_ref, mean_variance_hbm, sems.at[2]),
    ]
    width = params_ref.shape[1] // (CHIPS * CORES)
    for i, r in enumerate(ordered(GATHER_CHIPS)):
        here, there = pl.ds(i * width, width), pl.ds(r * width, width)
        copies.append(
            pltpu.make_async_copy(params_ref.at[:, here], params_hbm.at[:, there], sems.at[3 + i])
        )
    update_rms_ref[0] = scalars_ref[0, 0]
    mean_variance_ref[0] = scalars_ref[1, 0]
    for copy in copies:
        copy.start()
    for copy in copies:
        copy.wait()


def exchanged(blocks, axes, groups=None):
    return lax.all_to_all(blocks, axes, 0, 0, axis_index_groups=groups, tiled=True)


def shards(delta, counts, params, momentum):
    length = lax.axis_size(REP)
    rows, width = momentum.shape
    shape = functools.partial(jax.ShapeDtypeStruct, (rows, width))
    counts, delta, params = [
        pltpu.with_memory_space_constraint(a, pltpu.MemorySpace.HBM)
        for a in (counts, delta, params)
    ]
    blocks, own_params, weights = pl.pallas_call(
        split_kernel,
        in_specs=[HBM] * 3,
        out_specs=[VMEM] * 3,
        out_shape=[
            jax.ShapeDtypeStruct((length, rows, width), delta.dtype),
            shape(params.dtype),
            jax.ShapeDtypeStruct((length, LANES), jnp.float32),
        ],
        scratch_shapes=[pltpu.SMEM(counts.shape, counts.dtype), pltpu.SemaphoreType.DMA((length + 2,))],
        compiler_params=SMALL,
    )(counts, delta, params)
    blocks = exchanged(blocks, REP, [ordered(EXCHANGE_CHIPS)])
    mean, variance, totals = pl.pallas_call(
        moments_kernel,
        in_specs=[VMEM] * 2,
        out_specs=[VMEM] * 3,
        out_shape=[
            shape(jnp.float32),
            shape(jnp.float32),
            jax.ShapeDtypeStruct((lax.axis_size(LINE), 1, LANES), jnp.float32),
        ],
        compiler_params=SMALL,
    )(blocks, weights)
    line_totals = jnp.sum(exchanged(totals, LINE, [line_group()]), axis=0)
    groups = plane_groups()
    totals = jnp.broadcast_to(line_totals[None], (len(groups[0]), *line_totals.shape))
    totals = exchanged(totals, PLANE, groups)
    element_count = rows * width * length * lax.axis_size(SHARD)
    new_block, new_momentum, scalars = pl.pallas_call(
        functools.partial(update_kernel, element_count),
        in_specs=[VMEM] * 5,
        out_specs=[VMEM] * 3,
        out_shape=[
            shape(params.dtype),
            shape(jnp.float32),
            jax.ShapeDtypeStruct((2, LANES), jnp.float32),
        ],
        compiler_params=SMALL,
    )(totals, mean, variance, own_params, momentum)
    new_params = lax.all_gather(
        new_block, REP, axis_index_groups=[ordered(GATHER_CHIPS)], axis=1, tiled=True
    )
    scalar = jax.ShapeDtypeStruct((1,), jnp.float32)
    new_params, new_momentum, update_rms, mean_variance = pl.pallas_call(
        store_kernel,
        in_specs=[VMEM] * 3,
        out_specs=[HBM] * 4,
        out_shape=[
            jax.ShapeDtypeStruct(params.shape, params.dtype),
            shape(jnp.float32),
            scalar,
            scalar,
        ],
        scratch_shapes=[
            pltpu.SMEM((1,), jnp.float32),
            pltpu.SMEM((1,), jnp.float32),
            pltpu.SemaphoreType.DMA((3 + CHIPS * CORES,)),
        ],
        compiler_params=SMALL,
    )(new_params, new_momentum, scalars)
    return (new_params, new_momentum, update_rms[0], mean_variance[0])


def solution(mesh):
    finer = Mesh(
        mesh.devices.reshape(4, 2, 2, 4, 12), ("rep_0", "rep_1", "shard_0", "shard_1", "shard_2")
    )
    in_specs = (P(REP, SHARD, None), P(), P(SHARD, None), P(SHARD, REP))
    out_specs = (P(SHARD, None), P(SHARD, REP), P(), P())
    return jax.shard_map(
        shards, mesh=finer, in_specs=in_specs, out_specs=out_specs, check_vma=False
    )
```
